32 devices in a mesh: dp: 4 (over z), rows: 8 (over y, x, core).
Axes of the slice: x: 2, y: 2, z: 4, core: 2. Of those that a mesh axis runs over, the one named last changes fastest.
Arguments:
- latent: bfloat16 [8, 8, 64, 640], P('dp', 'rows'), may hold values from -16.25 to 16.25
- hidden: bfloat16 [8, 8, 64, 640], P('dp', 'rows'), may hold values from -16.25 to 16.25
- cotangent: bfloat16 [8, 8, 64, 640], P('dp', 'rows'), may hold values from -6 to 6
- filter_one: bfloat16 [9, 640, 640], P(None, 'dp', 'rows'), may hold values from -0.078125 to 0.078125
- filter_two: bfloat16 [9, 640, 640], P(None, 'dp', 'rows'), may hold values from -0.078125 to 0.078125
- gain_one: float32 [640], replicated, may hold values from 0.1 to 1.9
- shift_one: float32 [640], replicated, may hold values from -2.5 to 2.5
- gain_two: float32 [640], replicated, may hold values from 0.1 to 1.9
- shift_two: float32 [640], replicated, may hold values from -2.5 to 2.5
Outputs:
- latent_grad: bfloat16 [8, 8, 64, 640], P('dp', 'rows')
The draws below stay inside these ranges and needn't reach their ends.
All inputs are finite; a program needn't handle non-finite values.
Results may differ from the reference program's by a relative error of at most 0.0027.
Values may be sent and summed in bfloat16 or wider, within the bound.
A program may use at most 128 MiB of HBM per device.

```python
import jax
import jax.numpy as jnp
from jax import lax

GROUPS = 16
GSIZE = 40
WIDTH = 64
CH = 640
IMAGES = 8
HEIGHT = 8


def draw_field(key, salt):
    key = jax.random.fold_in(key, salt)
    key_noise, key_channel = jax.random.split(key, 2)
    height_pos = jnp.arange(HEIGHT, dtype=jnp.float32) / max(HEIGHT - 1, 1)
    row_scale = jnp.exp(jnp.log(3.0) * height_pos)[None, :, None, None]
    channel_scale = jnp.exp(jax.random.uniform(key_channel, (CH,), jnp.float32, jnp.log(0.1), 0.0))
    noise = jnp.clip(jax.random.normal(key_noise, (IMAGES, HEIGHT, WIDTH, CH), jnp.float32), -5.0, 5.0)
    field = noise * row_scale * channel_scale
    return field.astype(jnp.bfloat16)


def draw_latent(key, part):
    return draw_field(key, 11)


def draw_hidden(key, part):
    return draw_field(key, 23)


def draw_cotangent(key, part):
    key = jax.random.fold_in(key, 37)
    key_noise, key_offset = jax.random.split(key, 2)
    noise = jax.random.normal(key_noise, (IMAGES, HEIGHT, WIDTH, CH), jnp.float32)
    offset = jax.random.normal(key_offset, (IMAGES, 1, 1, CH), jnp.float32)
    field = jnp.clip(noise + offset, -6.0, 6.0)
    return field.astype(jnp.bfloat16)


def levels(key, dims, cuts, low, top_value):
    factor_of, own = 1.0, jax.random.fold_in(key, 6)
    for axis_at, blocks in cuts:
        draws = jnp.exp(jax.random.uniform(jax.random.fold_in(own, axis_at), (blocks,), jnp.float32, low / len(cuts), top_value / len(cuts)))
        factor_of = factor_of * jnp.repeat(draws, dims[axis_at] // blocks).reshape([-1 if axis == axis_at else 1 for axis in range(len(dims))])
    return factor_of


def centred(stream_key, extent, scale, most, cuts=(), held_as=jnp.bfloat16):
    level = levels(stream_key, extent, cuts, -0.22, 0.18) if cuts else 1.0
    values = jax.random.normal(stream_key, extent, jnp.float32) * scale * level
    return jnp.minimum(jnp.maximum(values, -most), most).astype(held_as)


def setup_inputs(seed: int = 0) -> dict:
    seeds = jax.random.split(jax.random.key(seed), 10)
    return {
        "latent": draw_latent(jax.random.fold_in(seeds[9], 71), 0),
        "hidden": draw_hidden(jax.random.fold_in(seeds[9], 71), 0),
        "cotangent": draw_cotangent(jax.random.fold_in(seeds[9], 71), 0),
        "filter_one": centred(seeds[3], (9, CH, CH), (9 * CH) ** -0.5, 0.078125, ((1, 4), (2, 8))),
        "filter_two": centred(seeds[4], (9, CH, CH), (9 * CH) ** -0.5, 0.078125, ((1, 4), (2, 8))),
        "gain_one": jnp.clip(1.0 + 0.18 * jax.random.normal(seeds[5], (CH,), jnp.float32), 0.1, 1.9),
        "shift_one": centred(seeds[6], (CH,), 0.5, 2.5, (), jnp.float32),
        "gain_two": jnp.clip(1.0 + 0.18 * jax.random.normal(seeds[7], (CH,), jnp.float32), 0.1, 1.9),
        "shift_two": centred(seeds[8], (CH,), 0.5, 2.5, (), jnp.float32),
    }


def group_sums(values):
    per_channel = lax.optimization_barrier(jnp.sum(values, axis=(1, 2)))
    return lax.optimization_barrier(jnp.sum(per_channel.reshape(per_channel.shape[0], GROUPS, -1), axis=2))

def expand_groups(moment):
    return jnp.repeat(moment, GSIZE, axis=1)[:, None, None, :]

def finish_stats(sum_plain, sum_square, number):
    average = sum_plain / number
    variance = sum_square / number - average * average
    return (average, lax.rsqrt(variance + 1e-05))

def norm_backward(field, stats, gain, shift, incoming, number):
    average, inverse = stats
    values = field.astype(jnp.float32)
    normed = (values - expand_groups(average)) * expand_groups(inverse)
    linear = normed * gain + shift
    logistic = jax.nn.sigmoid(linear)
    scaled = incoming * logistic * (1.0 + linear * (1.0 - logistic)) * gain
    first = group_sums(scaled) / number
    second = group_sums(scaled * normed) / number
    return expand_groups(inverse) * (scaled - expand_groups(first) - normed * expand_groups(second))

def conv_backward(gradient, weights):
    images, height, breadth, channels = gradient.shape
    padded = jnp.pad(gradient, ((0, 0), (1, 1), (1, 1), (0, 0)))
    result = jnp.zeros((images * height * breadth, channels), jnp.float32)
    for tap_index in range(9):
        down_step = tap_index // 3 - 1
        side_step = tap_index % 3 - 1
        window = padded[:, 1 - down_step:1 - down_step + height, 1 - side_step:1 - side_step + breadth, :]
        window = window.reshape(images * height * breadth, channels)
        result = result + jnp.dot(window, weights[tap_index].T, preferred_element_type=jnp.float32)
    return result.reshape(images, height, breadth, channels)

def reference(latent, hidden, cotangent, filter_one, filter_two, gain_one, shift_one, gain_two, shift_two):
    number = HEIGHT * WIDTH * GSIZE
    latent_values = latent.astype(jnp.float32)
    hidden_values = hidden.astype(jnp.float32)
    stats_one = finish_stats(group_sums(latent_values), group_sums(latent_values * latent_values), number)
    stats_two = finish_stats(group_sums(hidden_values), group_sums(hidden_values * hidden_values), number)
    back_two = conv_backward(cotangent, filter_two)
    hidden_grad = norm_backward(hidden, stats_two, gain_two, shift_two, back_two, number).astype(jnp.bfloat16)
    back_one = conv_backward(hidden_grad, filter_one)
    latent_part = norm_backward(latent, stats_one, gain_one, shift_one, back_one, number)
    return (cotangent.astype(jnp.float32) + latent_part).astype(jnp.bfloat16)
```

```python
import functools

import jax
import jax.numpy as jnp
from jax import lax
from jax.experimental import pallas as pl
from jax.experimental.pallas import tpu as pltpu
from jax.sharding import PartitionSpec as P

GROUPS = 16
GSIZE = 40
TAPS = 9
MESH = pl.DeviceIdType.MESH


def extended(block, sides, width):
    for axis, dim in sides:
        count = lax.axis_size(axis)
        forward = [(i, i + 1) for i in range(count - 1)]
        backward = [(target, source) for source, target in forward]
        low = lax.ppermute(
            lax.slice_in_dim(block, block.shape[dim] - width, None, axis=dim), axis, forward
        )
        high = lax.ppermute(lax.slice_in_dim(block, 0, width, axis=dim), axis, backward)
        block = jnp.concatenate([low, block, high], axis=dim)
    return block


def group_sums(values):
    per_channel = jnp.sum(values, axis=(1, 2))
    return jnp.sum(per_channel.reshape(per_channel.shape[0], GROUPS, -1), axis=2)


def expand_groups(moment):
    return jnp.repeat(moment, GSIZE, axis=1)[:, None, None, :]


def finish_stats(sum_plain, sum_square, number):
    average = sum_plain / number
    variance = sum_square / number - average * average
    return (average, lax.rsqrt(variance + 1e-05))


def reduced_stats(field, number):
    values = field.astype(jnp.float32)
    sum_plain, sum_square = lax.psum((group_sums(values), group_sums(values * values)), "rows")
    return finish_stats(sum_plain, sum_square, number)


def norm_backward(field, stats, gain, shift, incoming, number):
    average, inverse = stats
    values = field.astype(jnp.float32)
    normed = (values - expand_groups(average)) * expand_groups(inverse)
    linear = normed * gain + shift
    logistic = jax.nn.sigmoid(linear)
    scaled = incoming * logistic * (1.0 + linear * (1.0 - logistic)) * gain
    sum_first, sum_second = lax.psum((group_sums(scaled), group_sums(scaled * normed)), "rows")
    first = sum_first / number
    second = sum_second / number
    return expand_groups(inverse) * (scaled - expand_groups(first) - normed * expand_groups(second))


def conv_backward(gradient, weights):
    images, rows_here, breadth, channels = gradient.shape
    padded = extended(gradient, (("rows", 1),), 1)
    padded = jnp.pad(padded, ((0, 0), (0, 0), (1, 1), (0, 0)))
    pixels = images * rows_here * breadth
    shifted = []
    for tap_index in range(9):
        down_step = tap_index // 3 - 1
        side_step = tap_index % 3 - 1
        window = padded[
            :, 1 - down_step : 1 - down_step + rows_here, 1 - side_step : 1 - side_step + breadth, :
        ]
        shifted.append(window.reshape(pixels, channels))
    stacked = jnp.stack(shifted, axis=1)
    gathered = lax.all_gather(weights, "dp", axis=1, tiled=True)
    section = lax.all_gather(gathered, "rows", axis=2, tiled=True)
    columns = section.shape[2]
    window = stacked.reshape(pixels, 9 * columns)
    flat = jnp.transpose(section, (0, 2, 1)).reshape(9 * columns, section.shape[1])
    result = jnp.dot(window, flat, preferred_element_type=jnp.float32)
    return result.reshape(images, rows_here, breadth, channels)


def plain_body(
    latent, hidden, cotangent, filter_one, filter_two, gain_one, shift_one, gain_two, shift_two
):
    number = latent.shape[1] * lax.axis_size("rows") * latent.shape[2] * GSIZE
    stats_two = reduced_stats(hidden, number)
    back_two = conv_backward(cotangent, filter_two)
    hidden_grad = norm_backward(hidden, stats_two, gain_two, shift_two, back_two, number).astype(
        jnp.bfloat16
    )
    stats_one = reduced_stats(latent, number)
    back_one = conv_backward(hidden_grad, filter_one)
    latent_part = norm_backward(latent, stats_one, gain_one, shift_one, back_one, number)
    return (cotangent.astype(jnp.float32) + latent_part).astype(jnp.bfloat16)


def kernel(
    depth, rows, breadth,
    lat_ref, hid_ref, cot_ref, f1_ref, f2_ref, par_ref,
    out_ref,
    x_cot, x_hg, lat_t, hid_t, lat_b, hid_b, stage1, stage2, w1, w2, wt, y_ref, back, out_b, out_t,
    z_send, z_recv, w_send, w_recv, c_send, c_recv, g_send, g_recv,
    a_send, a_recv, o_send, o_recv,
):
    d = lax.axis_index("dp")
    r = lax.axis_index("rows")
    channels, lanes = x_cot.shape[1:]
    block = channels // rows
    images = lanes // breadth
    halves = rows // depth
    wide = w1.shape[2]
    number = rows * breadth * GSIZE

    def remote(src, dst, send, recv, **device):
        return pltpu.make_async_remote_copy(
            src_ref=src, dst_ref=dst, send_sem=send, recv_sem=recv,
            device_id=device, device_id_type=MESH,
        )

    barrier = pltpu.get_barrier_semaphore()
    for off in range(1, depth):
        pl.semaphore_signal(barrier, inc=1, device_id={"dp": lax.rem(d + off, depth)}, device_id_type=MESH)
    for off in range(1, rows):
        pl.semaphore_signal(barrier, inc=1, device_id={"rows": lax.rem(r + off, rows)}, device_id_type=MESH)

    x_cot[r] = cot_ref[...].T
    hid_t[...] = hid_ref[...].T
    lat_t[...] = lat_ref[...].T
    pl.semaphore_wait(barrier, depth - 1 + rows - 1)

    pending = []

    def start_z(which, src, stage):
        for off in (2, 1, 3) if depth == 4 else range(1, depth):
            to = lax.rem(d + off, depth)
            copy = remote(src, stage.at[d], z_send.at[which, to], z_recv.at[which, d], dp=to)
            copy.start()
            pending.append(copy)

    def start_exchange(which, src, dst):
        for off in range(1, rows):
            to = lax.rem(r + off, rows)
            copy = remote(
                src.at[pl.ds(to * block, block), :], dst.at[r],
                a_send.at[which, to], a_recv.at[which, r], rows=to,
            )
            copy.start()
            pending.append(copy)
        dst[r] = src[pl.ds(pl.multiple_of(r * block, block), block), :]

    def wait_exchange(which, src, dst):
        for off in range(1, rows):
            frm = lax.rem(r + off, rows)
            remote(src.at[pl.ds(0, block), :], dst.at[frm], a_send.at[which, frm], a_recv.at[which, frm], rows=frm).wait_recv()

    def send_pieces(which, origin, get, w, wait_own):
        for k in range(halves):
            to = origin * halves + k

            @pl.when(to != r)
            def _():
                remote(get(k), w.at[r], w_send.at[which, to], w_recv.at[which, r], rows=to).start()

            @pl.when(to == r)
            def _():
                w[r] = get(k)[...]

    def wait_piece_sends(which, src, w):
        for off in range(1, rows):
            to = lax.rem(r + off, rows)
            remote(src.at[0], w.at[r], w_send.at[which, to], w_recv.at[which, r], rows=to).wait_send()

    def relay_filters(which, stage, w):
        for off in (1, 3, 2) if depth == 4 else range(1, depth):
            origin = lax.rem(d + off, depth)
            remote(stage.at[origin], stage.at[origin], z_send.at[which, origin], z_recv.at[which, origin], dp=origin).wait_recv()
            send_pieces(which, origin, lambda k: stage.at[origin, k], w, False)

    def wait_filters(which, src, w):
        for off in range(1, rows):
            frm = lax.rem(r + off, rows)
            remote(src.at[0], w.at[frm], w_send.at[which, frm], w_recv.at[which, frm], rows=frm).wait_recv()

    parity = lax.rem(r, 2)
    sibling = r + 1 - 2 * parity

    def gather_send(at, send, recv):
        for off in range(1, rows // 2):
            to = lax.rem(r + 2 * off, rows)
            copy = remote(at(r), at(r), send.at[to], recv.at[r], rows=to)
            copy.start()
            pending.append(copy)
        copy = remote(at(r), at(r), send.at[sibling], recv.at[r], rows=sibling)
        copy.start()
        pending.append(copy)

    def gather_relay(at, send, recv):
        for off in range(1, rows // 2):
            frm = lax.rem(r + 2 * off, rows)
            remote(at(frm), at(frm), send.at[frm], recv.at[frm], rows=frm).wait_recv()
            twin = lax.rem(sibling + 2 * off, rows)
            copy = remote(at(frm), at(frm), send.at[twin], recv.at[frm], rows=sibling)
            copy.start()
            pending.append(copy)

    def gather_wait(at, send, recv):
        for off in range(0, rows // 2):
            frm = lax.rem(sibling + 2 * off, rows)
            remote(at(frm), at(frm), send.at[frm], recv.at[frm], rows=sibling).wait_recv()

    def cot_at(h):
        return x_cot.at[h]

    def hg_at(owner):
        return x_hg.at[:, pl.ds(pl.multiple_of(owner * block, block), block), :]

    start_z(0, f2_ref, stage2)
    gather_send(cot_at, c_send, c_recv)
    start_exchange(0, hid_t, hid_b)
    send_pieces(0, d, lambda k: f2_ref.at[k], w2, True)
    start_z(1, f1_ref, stage1)
    start_exchange(1, lat_t, lat_b)

    lane = lax.broadcasted_iota(jnp.int32, (1, lanes), 1)
    column = lax.rem(lane, breadth)
    image_of = lax.div(lane, breadth)
    groups = block // GSIZE

    def group_means(sums):
        per_lane = jnp.sum(sums.reshape(groups, GSIZE, lanes), axis=1)
        total = jnp.zeros_like(per_lane)
        for image in range(images):
            mine = image_of == image
            part = jnp.sum(jnp.where(mine, per_lane, 0.0), axis=1, keepdims=True)
            total = jnp.where(mine, part, total)
        total = total * (1.0 / number)
        return jnp.broadcast_to(total[:, None, :], (groups, GSIZE, lanes)).reshape(block, lanes)

    def stats(field):
        plain = jnp.zeros((block, lanes), jnp.float32)
        square = jnp.zeros((block, lanes), jnp.float32)
        for h in range(rows):
            values = field[h].astype(jnp.float32)
            plain += values
            square += values * values
        average = group_means(plain)
        variance = group_means(square) - average * average
        return average, lax.rsqrt(variance + 1e-05)

    params = par_ref[pl.ds(pl.multiple_of(r * block, block), block), :]

    def conv(x, w):
        wt[...] = w[...].reshape(channels, wide).T
        for h in range(0, rows, 2):
            pair = jnp.concatenate([x[h], x[h + 1]], axis=1)
            result = jnp.dot(wt[...], pair, preferred_element_type=jnp.float32)
            y_ref[h] = result[:, :lanes]
            y_ref[h + 1] = result[:, lanes:]

    def back_at(h):
        sums = []
        for side in range(3):
            total = None
            for down in range(3):
                source = h - (down - 1)
                if 0 <= source < rows:
                    tap = 3 * down + side
                    term = y_ref[source, tap * block : (tap + 1) * block, :]
                    total = term if total is None else total + term
            sums.append(total)
        left = jnp.where(column == breadth - 1, 0.0, pltpu.roll(sums[0], lanes - 1, 1))
        right = jnp.where(column == 0, 0.0, pltpu.roll(sums[2], 1, 1))
        return sums[1] + left + right

    def norm(field, moments, gain, shift, finish):
        average, inverse = moments
        sum_first = jnp.zeros((block, lanes), jnp.float32)
        sum_second = jnp.zeros((block, lanes), jnp.float32)
        for h in range(rows):
            normed = (field[h].astype(jnp.float32) - average) * inverse
            linear = normed * gain + shift
            logistic = 1.0 / (1.0 + jnp.exp(-linear))
            scaled = back_at(h) * logistic * (1.0 + linear * (1.0 - logistic)) * gain
            back[h] = scaled
            sum_first += scaled
            sum_second += scaled * normed
        first = group_means(sum_first)
        second = group_means(sum_second)
        for h in range(rows):
            normed = (field[h].astype(jnp.float32) - average) * inverse
            finish(h, inverse * (back[h] - first - normed * second))

    gather_relay(cot_at, c_send, c_recv)
    wait_exchange(0, hid_t, hid_b)
    moments_two = stats(hid_b)
    relay_filters(0, stage2, w2)
    send_pieces(1, d, lambda k: f1_ref.at[k], w1, True)
    wait_exchange(1, lat_t, lat_b)
    moments_one = stats(lat_b)
    gather_wait(cot_at, c_send, c_recv)
    wait_filters(0, f2_ref, w2)

    conv(x_cot, w2)
    mine = pl.ds(pl.multiple_of(r * block, block), block)

    def finish_two(h, value):
        x_hg[h, mine, :] = value.astype(jnp.bfloat16)

    norm(hid_b, moments_two, params[:, 2:3], params[:, 3:4], finish_two)
    gather_send(hg_at, g_send, g_recv)
    gather_relay(hg_at, g_send, g_recv)
    relay_filters(1, stage1, w1)
    gather_wait(hg_at, g_send, g_recv)
    wait_filters(1, f1_ref, w1)

    conv(x_hg, w1)

    def finish_one(h, value):
        out_b[h] = (x_cot[h, mine, :].astype(jnp.float32) + value).astype(jnp.bfloat16)

    norm(lat_b, moments_one, params[:, 0:1], params[:, 1:2], finish_one)
    for off in range(1, rows):
        to = lax.rem(r + off, rows)
        copy = remote(out_b.at[to], out_t.at[r], o_send.at[to], o_recv.at[r], rows=to)
        copy.start()
        pending.append(copy)
    out_t[r] = out_b[r]
    for off in range(1, rows):
        frm = lax.rem(r + off, rows)
        remote(out_b.at[frm], out_t.at[frm], o_send.at[frm], o_recv.at[frm], rows=frm).wait_recv()
    out_ref[...] = out_t[...].reshape(channels, lanes).T
    for copy in pending:
        copy.wait_send()
    wait_piece_sends(0, f2_ref, w2)
    wait_piece_sends(1, f1_ref, w1)


def arranged(weights, depth, rows):
    taps, inner, outer = weights.shape
    halves = rows // depth
    cut = weights.reshape(taps, halves, inner // halves, outer)
    flat = jnp.transpose(cut, (1, 3, 0, 2)).reshape(halves, outer, taps * (inner // halves))
    return jnp.pad(flat, ((0, 0), (0, 0), (0, -flat.shape[2] % 128)))


def kernel_body(
    depth, rows,
    latent, hidden, cotangent, filter_one, filter_two, gain_one, shift_one, gain_two, shift_two,
):
    images, _, breadth, channels = latent.shape
    lanes = images * breadth
    block = channels // rows
    halves = rows // depth
    f1 = arranged(filter_one, depth, rows)
    f2 = arranged(filter_two, depth, rows)
    wide = f1.shape[2]
    params = jnp.stack([gain_one, shift_one, gain_two, shift_two], axis=1)
    bf16, f32 = jnp.bfloat16, jnp.float32
    dma = pltpu.SemaphoreType.DMA
    out = pl.pallas_call(
        functools.partial(kernel, depth, rows, breadth),
        out_shape=jax.ShapeDtypeStruct((lanes, channels), bf16),
        in_specs=[pl.BlockSpec(memory_space=pltpu.VMEM)] * 6,
        out_specs=pl.BlockSpec(memory_space=pltpu.VMEM),
        scratch_shapes=[
            pltpu.VMEM((rows, channels, lanes), bf16),
            pltpu.VMEM((rows, channels, lanes), bf16),
            pltpu.VMEM((channels, lanes), bf16),
            pltpu.VMEM((channels, lanes), bf16),
            pltpu.VMEM((rows, block, lanes), bf16),
            pltpu.VMEM((rows, block, lanes), bf16),
            pltpu.VMEM((depth, halves, block, wide), bf16),
            pltpu.VMEM((depth, halves, block, wide), bf16),
            pltpu.VMEM((rows, block, wide), bf16),
            pltpu.VMEM((rows, block, wide), bf16),
            pltpu.VMEM((wide, channels), bf16),
            pltpu.VMEM((rows, wide, lanes), f32),
            pltpu.VMEM((rows, block, lanes), f32),
            pltpu.VMEM((rows, block, lanes), bf16),
            pltpu.VMEM((rows, block, lanes), bf16),
            dma((2, depth)), dma((2, depth)),
            dma((2, rows)), dma((2, rows)),
            dma((rows,)), dma((rows,)),
            dma((rows,)), dma((rows,)),
            dma((2, rows)), dma((2, rows)),
            dma((rows,)), dma((rows,)),
        ],
        compiler_params=pltpu.CompilerParams(collective_id=0, has_side_effects=True),
    )(
        latent.reshape(lanes, channels), hidden.reshape(lanes, channels),
        cotangent.reshape(lanes, channels), f1, f2, params,
    )
    return out.reshape(latent.shape)


def solution(mesh):
    depth, rows = mesh.shape["dp"], mesh.shape["rows"]
    in_specs = (
        P("dp", "rows", None, None),
        P("dp", "rows", None, None),
        P("dp", "rows", None, None),
        P(None, "dp", "rows"),
        P(None, "dp", "rows"),
        P(),
        P(),
        P(),
        P(),
    )

    def body(latent, *rest):
        images, rows_here, breadth, channels = latent.shape
        fits = (
            rows_here == 1
            and images * breadth == 128
            and rows % (2 * depth) == 0
            and channels % (rows * GSIZE) == 0
            and (channels // rows) % 16 == 0
            and channels % 128 == 0
        )
        if fits:
            return kernel_body(depth, rows, latent, *rest)
        return plain_body(latent, *rest)

    return jax.shard_map(
        body, mesh=mesh, in_specs=in_specs, out_specs=P("dp", "rows", None, None), check_vma=False
    )
```

```python
import functools

import jax
import jax.numpy as jnp
from jax import lax
from jax.experimental import pallas as pl
from jax.experimental.pallas import tpu as pltpu
from jax.sharding import PartitionSpec as P

GROUPS = 16
GSIZE = 40
TAPS = 9
MESH = pl.DeviceIdType.MESH


def extended(block, sides, width):
    for axis, dim in sides:
        count = lax.axis_size(axis)
        forward = [(i, i + 1) for i in range(count - 1)]
        backward = [(target, source) for source, target in forward]
        low = lax.ppermute(
            lax.slice_in_dim(block, block.shape[dim] - width, None, axis=dim), axis, forward
        )
        high = lax.ppermute(lax.slice_in_dim(block, 0, width, axis=dim), axis, backward)
        block = jnp.concatenate([low, block, high], axis=dim)
    return block


def group_sums(values):
    per_channel = jnp.sum(values, axis=(1, 2))
    return jnp.sum(per_channel.reshape(per_channel.shape[0], GROUPS, -1), axis=2)


def expand_groups(moment):
    return jnp.repeat(moment, GSIZE, axis=1)[:, None, None, :]


def finish_stats(sum_plain, sum_square, number):
    average = sum_plain / number
    variance = sum_square / number - average * average
    return (average, lax.rsqrt(variance + 1e-05))


def reduced_stats(field, number):
    values = field.astype(jnp.float32)
    sum_plain, sum_square = lax.psum((group_sums(values), group_sums(values * values)), "rows")
    return finish_stats(sum_plain, sum_square, number)


def norm_backward(field, stats, gain, shift, incoming, number):
    average, inverse = stats
    values = field.astype(jnp.float32)
    normed = (values - expand_groups(average)) * expand_groups(inverse)
    linear = normed * gain + shift
    logistic = jax.nn.sigmoid(linear)
    scaled = incoming * logistic * (1.0 + linear * (1.0 - logistic)) * gain
    sum_first, sum_second = lax.psum((group_sums(scaled), group_sums(scaled * normed)), "rows")
    first = sum_first / number
    second = sum_second / number
    return expand_groups(inverse) * (scaled - expand_groups(first) - normed * expand_groups(second))


def conv_backward(gradient, weights):
    images, rows_here, breadth, channels = gradient.shape
    padded = extended(gradient, (("rows", 1),), 1)
    padded = jnp.pad(padded, ((0, 0), (0, 0), (1, 1), (0, 0)))
    pixels = images * rows_here * breadth
    shifted = []
    for tap_index in range(9):
        down_step = tap_index // 3 - 1
        side_step = tap_index % 3 - 1
        window = padded[
            :, 1 - down_step : 1 - down_step + rows_here, 1 - side_step : 1 - side_step + breadth, :
        ]
        shifted.append(window.reshape(pixels, channels))
    stacked = jnp.stack(shifted, axis=1)
    gathered = lax.all_gather(weights, "dp", axis=1, tiled=True)
    section = lax.all_gather(gathered, "rows", axis=2, tiled=True)
    columns = section.shape[2]
    window = stacked.reshape(pixels, 9 * columns)
    flat = jnp.transpose(section, (0, 2, 1)).reshape(9 * columns, section.shape[1])
    result = jnp.dot(window, flat, preferred_element_type=jnp.float32)
    return result.reshape(images, rows_here, breadth, channels)


def plain_body(
    latent, hidden, cotangent, filter_one, filter_two, gain_one, shift_one, gain_two, shift_two
):
    number = latent.shape[1] * lax.axis_size("rows") * latent.shape[2] * GSIZE
    stats_two = reduced_stats(hidden, number)
    back_two = conv_backward(cotangent, filter_two)
    hidden_grad = norm_backward(hidden, stats_two, gain_two, shift_two, back_two, number).astype(
        jnp.bfloat16
    )
    stats_one = reduced_stats(latent, number)
    back_one = conv_backward(hidden_grad, filter_one)
    latent_part = norm_backward(latent, stats_one, gain_one, shift_one, back_one, number)
    return (cotangent.astype(jnp.float32) + latent_part).astype(jnp.bfloat16)


def kernel(
    depth, rows, breadth,
    lat_ref, hid_ref, cot_ref, raw1, raw2, gain1, shift1, gain2, shift2,
    out_ref,
    x_cot, x_hg, lat_t, hid_t, lat_b, hid_b, stage1, stage2, w1, w2, wt, y_ref, back, out_b, out_t,
    f1_ref, f2_ref, par_ref,
    z_send, z_recv, w_send, w_recv, c_send, c_recv, g_send, g_recv,
    a_send, a_recv, o_send, o_recv,
):
    d = lax.axis_index("dp")
    r = lax.axis_index("rows")
    channels, lanes = x_cot.shape[1:]
    block = channels // rows
    images = lanes // breadth
    halves = rows // depth
    wide = w1.shape[2]
    number = rows * breadth * GSIZE

    def place(index):
        return index + lax.rem(index, 2) * (rows - 2 * index)

    def rows_of(index):
        return pl.ds(pl.multiple_of(place(index) * block, block), block)

    def arrange(raw, ready):
        for k in range(halves):
            ready[k, :, TAPS * block :] = jnp.zeros((block, wide - TAPS * block), jnp.bfloat16)
        for tap in range(TAPS):
            turned = raw[tap].T
            for k in range(halves):
                ready[k, :, tap * block : (tap + 1) * block] = turned[:, k * block : (k + 1) * block]

    def remote(src, dst, send, recv, **device):
        return pltpu.make_async_remote_copy(
            src_ref=src, dst_ref=dst, send_sem=send, recv_sem=recv,
            device_id=device, device_id_type=MESH,
        )

    barrier = pltpu.get_barrier_semaphore()
    for off in range(1, depth):
        pl.semaphore_signal(barrier, inc=1, device_id={"dp": lax.rem(d + off, depth)}, device_id_type=MESH)
    for off in range(1, rows):
        pl.semaphore_signal(barrier, inc=1, device_id={"rows": lax.rem(r + off, rows)}, device_id_type=MESH)

    arrange(raw2, f2_ref)
    x_cot[r] = cot_ref[...].T
    hid_t[...] = hid_ref[...].T
    lat_t[...] = lat_ref[...].T
    pl.semaphore_wait(barrier, depth - 1 + rows - 1)

    pending = []

    def z_hop(which, src, stage, origin, way):
        to = d + 1 - 2 * way
        return remote(src, stage.at[origin], z_send.at[which, way, origin], z_recv.at[which, origin], dp=to)

    def start_z(which, src, stage):
        @pl.when(d < depth - 1)
        def _():
            z_hop(which, src, stage, d, 0).start()

        @pl.when(d > 0)
        def _():
            z_hop(which, src, stage, d, 1).start()

    def wait_z_sends(which, src, stage):
        for origin in range(depth):
            @pl.when((d < depth - 1) & (origin <= d))
            def _():
                z_hop(which, src, stage, origin, 0).wait_send()

            @pl.when((d > 0) & (origin >= d))
            def _():
                z_hop(which, src, stage, origin, 1).wait_send()

    def start_exchange(which, src, dst):
        for off in range(1, rows):
            to = lax.rem(r + off, rows)
            copy = remote(
                src.at[rows_of(to), :], dst.at[r],
                a_send.at[which, to], a_recv.at[which, r], rows=to,
            )
            copy.start()
            pending.append(copy)
        dst[r] = src[rows_of(r), :]

    def wait_exchange(which, src, dst):
        for off in range(1, rows):
            frm = lax.rem(r + off, rows)
            remote(src.at[pl.ds(0, block), :], dst.at[frm], a_send.at[which, frm], a_recv.at[which, frm], rows=frm).wait_recv()

    def send_pieces(which, origin, get, w, wait_own):
        for k in range(halves):
            to = place(origin * halves + k)

            @pl.when(to != r)
            def _():
                remote(get(k), w.at[r], w_send.at[which, to], w_recv.at[which, r], rows=to).start()

            @pl.when(to == r)
            def _():
                w[r] = get(k)[...]

    def wait_piece_sends(which, src, w):
        for off in range(1, rows):
            to = lax.rem(r + off, rows)
            remote(src.at[0], w.at[r], w_send.at[which, to], w_recv.at[which, r], rows=to).wait_send()

    def relay_filters(which, stage, w, off):
        @pl.when(d >= off)
        def _():
            origin = d - off
            hop = z_hop(which, stage.at[origin], stage, origin, 0)
            hop.wait_recv()

            @pl.when(d < depth - 1)
            def _():
                hop.start()

            send_pieces(which, origin, lambda k: stage.at[origin, k], w, False)

        @pl.when(d + off < depth)
        def _():
            origin = d + off
            hop = z_hop(which, stage.at[origin], stage, origin, 1)
            hop.wait_recv()

            @pl.when(d > 0)
            def _():
                hop.start()

            send_pieces(which, origin, lambda k: stage.at[origin, k], w, False)

    def wait_filters(which, src, w):
        for off in range(1, rows):
            frm = lax.rem(r + off, rows)
            remote(src.at[0], w.at[frm], w_send.at[which, frm], w_recv.at[which, frm], rows=frm).wait_recv()

    parity = lax.rem(r, 2)
    sibling = r + 1 - 2 * parity

    def gather_send(at, send, recv):
        for off in range(1, rows // 2):
            to = lax.rem(r + 2 * off, rows)
            copy = remote(at(r), at(r), send.at[to], recv.at[r], rows=to)
            copy.start()
            pending.append(copy)
        copy = remote(at(r), at(r), send.at[sibling], recv.at[r], rows=sibling)
        copy.start()
        pending.append(copy)

    def gather_relay(at, send, recv):
        for off in range(1, rows // 2):
            frm = lax.rem(r + 2 * off, rows)
            remote(at(frm), at(frm), send.at[frm], recv.at[frm], rows=frm).wait_recv()
            twin = lax.rem(sibling + 2 * off, rows)
            copy = remote(at(frm), at(frm), send.at[twin], recv.at[frm], rows=sibling)
            copy.start()
            pending.append(copy)

    def gather_wait(at, send, recv):
        for off in range(0, rows // 2):
            frm = lax.rem(sibling + 2 * off, rows)
            remote(at(frm), at(frm), send.at[frm], recv.at[frm], rows=sibling).wait_recv()

    def cot_at(h):
        return x_cot.at[h]

    def hg_at(owner):
        return x_hg.at[:, rows_of(owner), :]

    start_z(0, f2_ref, stage2)
    gather_send(cot_at, c_send, c_recv)
    start_exchange(0, hid_t, hid_b)
    send_pieces(0, d, lambda k: f2_ref.at[k], w2, True)
    start_exchange(1, lat_t, lat_b)
    arrange(raw1, f1_ref)
    raw_params = [gain1[...], shift1[...], gain2[...], shift2[...]]
    par_ref[...] = jnp.concatenate(raw_params + raw_params, axis=0).T

    lane = lax.broadcasted_iota(jnp.int32, (1, lanes), 1)
    column = lax.rem(lane, breadth)
    image_of = lax.div(lane, breadth)
    groups = block // GSIZE

    def group_means(sums):
        per_lane = jnp.sum(sums.reshape(groups, GSIZE, lanes), axis=1)
        total = jnp.zeros_like(per_lane)
        for image in range(images):
            mine = image_of == image
            part = jnp.sum(jnp.where(mine, per_lane, 0.0), axis=1, keepdims=True)
            total = jnp.where(mine, part, total)
        total = total * (1.0 / number)
        return jnp.broadcast_to(total[:, None, :], (groups, GSIZE, lanes)).reshape(block, lanes)

    def stats(field):
        plain = jnp.zeros((block, lanes), jnp.float32)
        square = jnp.zeros((block, lanes), jnp.float32)
        for h in range(rows):
            values = field[h].astype(jnp.float32)
            plain += values
            square += values * values
        average = group_means(plain)
        variance = group_means(square) - average * average
        return average, lax.rsqrt(variance + 1e-05)

    params = par_ref[rows_of(r), :]

    def conv(x, w):
        wt[...] = w[...].reshape(channels, wide).T
        for h in range(0, rows, 2):
            pair = jnp.concatenate([x[h], x[h + 1]], axis=1)
            result = jnp.dot(wt[...], pair, preferred_element_type=jnp.float32)
            y_ref[h] = result[:, :lanes]
            y_ref[h + 1] = result[:, lanes:]

    def back_at(h):
        sums = []
        for side in range(3):
            total = None
            for down in range(3):
                source = h - (down - 1)
                if 0 <= source < rows:
                    tap = 3 * down + side
                    term = y_ref[source, tap * block : (tap + 1) * block, :]
                    total = term if total is None else total + term
            sums.append(total)
        left = jnp.where(column == breadth - 1, 0.0, pltpu.roll(sums[0], lanes - 1, 1))
        right = jnp.where(column == 0, 0.0, pltpu.roll(sums[2], 1, 1))
        return sums[1] + left + right

    def norm(field, moments, gain, shift, finish):
        average, inverse = moments
        sum_first = jnp.zeros((block, lanes), jnp.float32)
        sum_second = jnp.zeros((block, lanes), jnp.float32)
        for h in range(rows):
            normed = (field[h].astype(jnp.float32) - average) * inverse
            linear = normed * gain + shift
            logistic = 1.0 / (1.0 + jnp.exp(-linear))
            scaled = back_at(h) * logistic * (1.0 + linear * (1.0 - logistic)) * gain
            back[h] = scaled
            sum_first += scaled
            sum_second += scaled * normed
        first = group_means(sum_first)
        second = group_means(sum_second)
        for h in range(rows):
            normed = (field[h].astype(jnp.float32) - average) * inverse
            finish(h, inverse * (back[h] - first - normed * second))

    gather_relay(cot_at, c_send, c_recv)
    relay_filters(0, stage2, w2, 1)
    wait_exchange(0, hid_t, hid_b)
    moments_two = stats(hid_b)
    wait_exchange(1, lat_t, lat_b)
    moments_one = stats(lat_b)
    for off in range(2, depth):
        relay_filters(0, stage2, w2, off)
    start_z(1, f1_ref, stage1)
    gather_wait(cot_at, c_send, c_recv)
    wait_filters(0, f2_ref, w2)

    conv(x_cot, w2)
    mine = rows_of(r)

    def finish_two(h, value):
        x_hg[h, mine, :] = value.astype(jnp.bfloat16)

    norm(hid_b, moments_two, params[:, 2:3], params[:, 3:4], finish_two)
    gather_send(hg_at, g_send, g_recv)
    send_pieces(1, d, lambda k: f1_ref.at[k], w1, True)
    relay_filters(1, stage1, w1, 1)
    gather_relay(hg_at, g_send, g_recv)
    for off in range(2, depth):
        relay_filters(1, stage1, w1, off)
    gather_wait(hg_at, g_send, g_recv)
    wait_filters(1, f1_ref, w1)

    conv(x_hg, w1)

    def finish_one(h, value):
        out_b[h] = (x_cot[h, mine, :].astype(jnp.float32) + value).astype(jnp.bfloat16)

    norm(lat_b, moments_one, params[:, 0:1], params[:, 1:2], finish_one)
    for off in range(1, rows):
        to = lax.rem(r + off, rows)
        copy = remote(out_b.at[to], out_t.at[place(r)], o_send.at[to], o_recv.at[r], rows=to)
        copy.start()
        pending.append(copy)
    out_t[place(r)] = out_b[r]
    for off in range(1, rows):
        frm = lax.rem(r + off, rows)
        remote(out_b.at[frm], out_t.at[place(frm)], o_send.at[frm], o_recv.at[frm], rows=frm).wait_recv()
    out_ref[...] = out_t[...].reshape(channels, lanes).T
    for copy in pending:
        copy.wait_send()
    wait_z_sends(0, f2_ref, stage2)
    wait_z_sends(1, f1_ref, stage1)
    wait_piece_sends(0, f2_ref, w2)
    wait_piece_sends(1, f1_ref, w1)


def kernel_body(
    depth, rows,
    latent, hidden, cotangent, filter_one, filter_two, gain_one, shift_one, gain_two, shift_two,
):
    images, _, breadth, channels = latent.shape
    lanes = images * breadth
    block = channels // rows
    halves = rows // depth
    wide = -(-TAPS * block // 128) * 128
    bf16, f32 = jnp.bfloat16, jnp.float32
    dma = pltpu.SemaphoreType.DMA
    out = pl.pallas_call(
        functools.partial(kernel, depth, rows, breadth),
        out_shape=jax.ShapeDtypeStruct((lanes, channels), bf16),
        in_specs=[pl.BlockSpec(memory_space=pltpu.VMEM)] * 9,
        out_specs=pl.BlockSpec(memory_space=pltpu.VMEM),
        scratch_shapes=[
            pltpu.VMEM((rows, channels, lanes), bf16),
            pltpu.VMEM((rows, channels, lanes), bf16),
            pltpu.VMEM((channels, lanes), bf16),
            pltpu.VMEM((channels, lanes), bf16),
            pltpu.VMEM((rows, block, lanes), bf16),
            pltpu.VMEM((rows, block, lanes), bf16),
            pltpu.VMEM((depth, halves, block, wide), bf16),
            pltpu.VMEM((depth, halves, block, wide), bf16),
            pltpu.VMEM((rows, block, wide), bf16),
            pltpu.VMEM((rows, block, wide), bf16),
            pltpu.VMEM((wide, channels), bf16),
            pltpu.VMEM((rows, wide, lanes), f32),
            pltpu.VMEM((rows, block, lanes), f32),
            pltpu.VMEM((rows, block, lanes), bf16),
            pltpu.VMEM((rows, block, lanes), bf16),
            pltpu.VMEM((halves, block, wide), bf16),
            pltpu.VMEM((halves, block, wide), bf16),
            pltpu.VMEM((channels, 8), f32),
            dma((2, 2, depth)), dma((2, depth)),
            dma((2, rows)), dma((2, rows)),
            dma((rows,)), dma((rows,)),
            dma((rows,)), dma((rows,)),
            dma((2, rows)), dma((2, rows)),
            dma((rows,)), dma((rows,)),
        ],
        compiler_params=pltpu.CompilerParams(collective_id=0, has_side_effects=True),
    )(
        latent.reshape(lanes, channels), hidden.reshape(lanes, channels),
        cotangent.reshape(lanes, channels), filter_one, filter_two,
        *(vector.reshape(1, channels) for vector in (gain_one, shift_one, gain_two, shift_two)),
    )
    return out.reshape(latent.shape)


def solution(mesh):
    depth, rows = mesh.shape["dp"], mesh.shape["rows"]
    in_specs = (
        P("dp", "rows", None, None),
        P("dp", "rows", None, None),
        P("dp", "rows", None, None),
        P(None, "dp", "rows"),
        P(None, "dp", "rows"),
        P(),
        P(),
        P(),
        P(),
    )

    def body(latent, *rest):
        images, rows_here, breadth, channels = latent.shape
        fits = (
            rows_here == 1
            and images * breadth == 128
            and rows == 2 * depth
            and rows % 2 == 0
            and channels % (rows * GSIZE) == 0
            and (channels // rows) % 16 == 0
            and channels % 128 == 0
        )
        if fits:
            return kernel_body(depth, rows, latent, *rest)
        return plain_body(latent, *rest)

    return jax.shard_map(
        body, mesh=mesh, in_specs=in_specs, out_specs=P("dp", "rows", None, None), check_vma=False
    )
```

```python
import functools

import jax
import jax.numpy as jnp
from jax import lax
from jax.experimental import pallas as pl
from jax.experimental.pallas import tpu as pltpu
from jax.sharding import PartitionSpec as P

GROUPS = 16
GSIZE = 40
TAPS = 9
MESH = pl.DeviceIdType.MESH


def extended(block, sides, width):
    for axis, dim in sides:
        count = lax.axis_size(axis)
        forward = [(i, i + 1) for i in range(count - 1)]
        backward = [(target, source) for source, target in forward]
        low = lax.ppermute(
            lax.slice_in_dim(block, block.shape[dim] - width, None, axis=dim), axis, forward
        )
        high = lax.ppermute(lax.slice_in_dim(block, 0, width, axis=dim), axis, backward)
        block = jnp.concatenate([low, block, high], axis=dim)
    return block


def group_sums(values):
    per_channel = jnp.sum(values, axis=(1, 2))
    return jnp.sum(per_channel.reshape(per_channel.shape[0], GROUPS, -1), axis=2)


def expand_groups(moment):
    return jnp.repeat(moment, GSIZE, axis=1)[:, None, None, :]


def finish_stats(sum_plain, sum_square, number):
    average = sum_plain / number
    variance = sum_square / number - average * average
    return (average, lax.rsqrt(variance + 1e-05))


def reduced_stats(field, number):
    values = field.astype(jnp.float32)
    sum_plain, sum_square = lax.psum((group_sums(values), group_sums(values * values)), "rows")
    return finish_stats(sum_plain, sum_square, number)


def norm_backward(field, stats, gain, shift, incoming, number):
    average, inverse = stats
    values = field.astype(jnp.float32)
    normed = (values - expand_groups(average)) * expand_groups(inverse)
    linear = normed * gain + shift
    logistic = jax.nn.sigmoid(linear)
    scaled = incoming * logistic * (1.0 + linear * (1.0 - logistic)) * gain
    sum_first, sum_second = lax.psum((group_sums(scaled), group_sums(scaled * normed)), "rows")
    first = sum_first / number
    second = sum_second / number
    return expand_groups(inverse) * (scaled - expand_groups(first) - normed * expand_groups(second))


def conv_backward(gradient, weights):
    images, rows_here, breadth, channels = gradient.shape
    padded = extended(gradient, (("rows", 1),), 1)
    padded = jnp.pad(padded, ((0, 0), (0, 0), (1, 1), (0, 0)))
    pixels = images * rows_here * breadth
    shifted = []
    for tap_index in range(9):
        down_step = tap_index // 3 - 1
        side_step = tap_index % 3 - 1
        window = padded[
            :, 1 - down_step : 1 - down_step + rows_here, 1 - side_step : 1 - side_step + breadth, :
        ]
        shifted.append(window.reshape(pixels, channels))
    stacked = jnp.stack(shifted, axis=1)
    gathered = lax.all_gather(weights, "dp", axis=1, tiled=True)
    section = lax.all_gather(gathered, "rows", axis=2, tiled=True)
    columns = section.shape[2]
    window = stacked.reshape(pixels, 9 * columns)
    flat = jnp.transpose(section, (0, 2, 1)).reshape(9 * columns, section.shape[1])
    result = jnp.dot(window, flat, preferred_element_type=jnp.float32)
    return result.reshape(images, rows_here, breadth, channels)


def plain_body(
    latent, hidden, cotangent, filter_one, filter_two, gain_one, shift_one, gain_two, shift_two
):
    number = latent.shape[1] * lax.axis_size("rows") * latent.shape[2] * GSIZE
    stats_two = reduced_stats(hidden, number)
    back_two = conv_backward(cotangent, filter_two)
    hidden_grad = norm_backward(hidden, stats_two, gain_two, shift_two, back_two, number).astype(
        jnp.bfloat16
    )
    stats_one = reduced_stats(latent, number)
    back_one = conv_backward(hidden_grad, filter_one)
    latent_part = norm_backward(latent, stats_one, gain_one, shift_one, back_one, number)
    return (cotangent.astype(jnp.float32) + latent_part).astype(jnp.bfloat16)


def kernel(
    depth, rows, breadth,
    lat_ref, hid_ref, cot_ref, raw1, raw2, gain1, shift1, gain2, shift2,
    out_ref,
    x_cot, x_hg, lat_t, hid_t, lat_b, hid_b, stage1, stage2, w1, w2, wt, y_ref, back, out_b, out_t,
    f1_ref, f2_ref, par_ref,
    z_send, z_recv, w_send, w_recv, c_send, c_recv, g_send, g_recv,
    a_send, a_recv, o_send, o_recv,
):
    d = lax.axis_index("dp")
    r = lax.axis_index("rows")
    channels, lanes = x_cot.shape[1:]
    block = channels // rows
    images = lanes // breadth
    halves = rows // depth
    wide = w1.shape[2]
    number = rows * breadth * GSIZE

    def place(index):
        return index + lax.rem(index, 2) * (rows - 2 * index)

    def rows_of(index):
        return pl.ds(pl.multiple_of(place(index) * block, block), block)

    def arrange(raw, ready):
        for k in range(halves):
            ready[k, :, TAPS * block :] = jnp.zeros((block, wide - TAPS * block), jnp.bfloat16)
        for tap in range(TAPS):
            turned = raw[tap].T
            for k in range(halves):
                ready[k, :, tap * block : (tap + 1) * block] = turned[:, k * block : (k + 1) * block]

    def remote(src, dst, send, recv, **device):
        return pltpu.make_async_remote_copy(
            src_ref=src, dst_ref=dst, send_sem=send, recv_sem=recv,
            device_id=device, device_id_type=MESH,
        )

    barrier = pltpu.get_barrier_semaphore()
    for off in range(1, depth):
        pl.semaphore_signal(barrier, inc=1, device_id={"dp": lax.rem(d + off, depth)}, device_id_type=MESH)
    for off in range(1, rows):
        pl.semaphore_signal(barrier, inc=1, device_id={"rows": lax.rem(r + off, rows)}, device_id_type=MESH)

    arrange(raw2, f2_ref)
    x_cot[r] = cot_ref[...].T
    hid_t[...] = hid_ref[...].T
    lat_t[...] = lat_ref[...].T
    pl.semaphore_wait(barrier, depth - 1 + rows - 1)

    pending = []

    def z_hop(which, src, stage, origin, k, way):
        to = d + 1 - 2 * way
        return remote(
            src, stage.at[origin, k], z_send.at[which, way, origin, k], z_recv.at[which, origin, k], dp=to
        )

    def start_z(which, src, stage):
        for k in range(halves):
            @pl.when(d < depth - 1)
            def _():
                z_hop(which, src.at[k], stage, d, k, 0).start()

            @pl.when(d > 0)
            def _():
                z_hop(which, src.at[k], stage, d, k, 1).start()

    def wait_z_sends(which, src, stage):
        for origin in range(depth):
            for k in range(halves):
                @pl.when((d < depth - 1) & (origin <= d))
                def _():
                    z_hop(which, src.at[k], stage, origin, k, 0).wait_send()

                @pl.when((d > 0) & (origin >= d))
                def _():
                    z_hop(which, src.at[k], stage, origin, k, 1).wait_send()

    def start_exchange(which, src, dst):
        for off in range(1, rows):
            to = lax.rem(r + off, rows)
            copy = remote(
                src.at[rows_of(to), :], dst.at[r],
                a_send.at[which, to], a_recv.at[which, r], rows=to,
            )
            copy.start()
            pending.append(copy)
        dst[r] = src[rows_of(r), :]

    def wait_exchange(which, src, dst):
        for off in range(1, rows):
            frm = lax.rem(r + off, rows)
            remote(src.at[pl.ds(0, block), :], dst.at[frm], a_send.at[which, frm], a_recv.at[which, frm], rows=frm).wait_recv()

    def send_piece(which, origin, k, piece, w):
        to = place(origin * halves + k)

        @pl.when(to != r)
        def _():
            remote(piece, w.at[r], w_send.at[which, to], w_recv.at[which, r], rows=to).start()

        @pl.when(to == r)
        def _():
            w[r] = piece[...]

    def send_own(which, src, w):
        for k in range(halves):
            send_piece(which, d, k, src.at[k], w)

    def wait_piece_sends(which, src, w):
        for off in range(1, rows):
            to = lax.rem(r + off, rows)
            remote(src.at[0], w.at[r], w_send.at[which, to], w_recv.at[which, r], rows=to).wait_send()

    def relay_filters(which, stage, w, off):
        for k in range(halves):
            for way in range(2):
                origin = d - off if way == 0 else d + off

                @pl.when((origin >= 0) & (origin < depth))
                def _():
                    hop = z_hop(which, stage.at[origin, k], stage, origin, k, way)
                    hop.wait_recv()

                    @pl.when((d < depth - 1) if way == 0 else (d > 0))
                    def _():
                        hop.start()

                    send_piece(which, origin, k, stage.at[origin, k], w)

    def wait_filters(which, src, w):
        for off in range(1, rows):
            frm = lax.rem(r + off, rows)
            remote(src.at[0], w.at[frm], w_send.at[which, frm], w_recv.at[which, frm], rows=frm).wait_recv()

    parity = lax.rem(r, 2)
    sibling = r + 1 - 2 * parity

    def gather_send(at, send, recv):
        for off in range(1, rows // 2):
            to = lax.rem(r + 2 * off, rows)
            copy = remote(at(r), at(r), send.at[to], recv.at[r], rows=to)
            copy.start()
            pending.append(copy)
        copy = remote(at(r), at(r), send.at[sibling], recv.at[r], rows=sibling)
        copy.start()
        pending.append(copy)

    def gather_relay(at, send, recv):
        for off in range(1, rows // 2):
            frm = lax.rem(r + 2 * off, rows)
            remote(at(frm), at(frm), send.at[frm], recv.at[frm], rows=frm).wait_recv()
            twin = lax.rem(sibling + 2 * off, rows)
            copy = remote(at(frm), at(frm), send.at[twin], recv.at[frm], rows=sibling)
            copy.start()
            pending.append(copy)

    def gather_wait(at, send, recv):
        for off in range(0, rows // 2):
            frm = lax.rem(sibling + 2 * off, rows)
            remote(at(frm), at(frm), send.at[frm], recv.at[frm], rows=sibling).wait_recv()

    def cot_at(h):
        return x_cot.at[h]

    def hg_at(owner):
        return x_hg.at[:, rows_of(owner), :]

    start_z(0, f2_ref, stage2)
    gather_send(cot_at, c_send, c_recv)
    start_exchange(0, hid_t, hid_b)
    send_own(0, f2_ref, w2)
    arrange(raw1, f1_ref)
    raw_params = [p[...].reshape(1, channels) for p in (gain1, shift1, gain2, shift2)]
    par_ref[...] = jnp.concatenate(raw_params + raw_params, axis=0).T

    lane = lax.broadcasted_iota(jnp.int32, (1, lanes), 1)
    column = lax.rem(lane, breadth)
    image_of = lax.div(lane, breadth)
    groups = block // GSIZE

    def group_means(sums):
        per_lane = jnp.sum(sums.reshape(groups, GSIZE, lanes), axis=1)
        total = jnp.zeros_like(per_lane)
        for image in range(images):
            mine = image_of == image
            part = jnp.sum(jnp.where(mine, per_lane, 0.0), axis=1, keepdims=True)
            total = jnp.where(mine, part, total)
        total = total * (1.0 / number)
        return jnp.broadcast_to(total[:, None, :], (groups, GSIZE, lanes)).reshape(block, lanes)

    def stats(field):
        plain = jnp.zeros((block, lanes), jnp.float32)
        square = jnp.zeros((block, lanes), jnp.float32)
        for h in range(rows):
            values = field[h].astype(jnp.float32)
            plain += values
            square += values * values
        average = group_means(plain)
        variance = group_means(square) - average * average
        return average, lax.rsqrt(variance + 1e-05)

    params = par_ref[rows_of(r), :]

    def conv(x, w):
        wt[...] = w[...].reshape(channels, wide).T
        for h in range(0, rows, 2):
            pair = jnp.concatenate([x[h], x[h + 1]], axis=1)
            result = jnp.dot(wt[...], pair, preferred_element_type=jnp.float32)
            y_ref[h] = result[:, :lanes]
            y_ref[h + 1] = result[:, lanes:]

    def back_at(h):
        sums = []
        for side in range(3):
            total = None
            for down in range(3):
                source = h - (down - 1)
                if 0 <= source < rows:
                    tap = 3 * down + side
                    term = y_ref[source, tap * block : (tap + 1) * block, :]
                    total = term if total is None else total + term
            sums.append(total)
        left = jnp.where(column == breadth - 1, 0.0, pltpu.roll(sums[0], lanes - 1, 1))
        right = jnp.where(column == 0, 0.0, pltpu.roll(sums[2], 1, 1))
        return sums[1] + left + right

    def norm(field, moments, gain, shift, finish):
        average, inverse = moments
        sum_first = jnp.zeros((block, lanes), jnp.float32)
        sum_second = jnp.zeros((block, lanes), jnp.float32)
        for h in range(rows):
            normed = (field[h].astype(jnp.float32) - average) * inverse
            linear = normed * gain + shift
            logistic = 1.0 / (1.0 + jnp.exp(-linear))
            scaled = back_at(h) * logistic * (1.0 + linear * (1.0 - logistic)) * gain
            back[h] = scaled
            sum_first += scaled
            sum_second += scaled * normed
        first = group_means(sum_first)
        second = group_means(sum_second)
        for h in range(rows):
            normed = (field[h].astype(jnp.float32) - average) * inverse
            finish(h, inverse * (back[h] - first - normed * second))

    relay_filters(0, stage2, w2, 1)
    gather_relay(cot_at, c_send, c_recv)
    start_exchange(1, lat_t, lat_b)
    relay_filters(0, stage2, w2, 2)
    wait_exchange(0, hid_t, hid_b)
    moments_two = stats(hid_b)
    start_z(1, f1_ref, stage1)
    for off in range(3, depth):
        relay_filters(0, stage2, w2, off)
    gather_wait(cot_at, c_send, c_recv)
    wait_filters(0, f2_ref, w2)

    conv(x_cot, w2)
    send_own(1, f1_ref, w1)
    relay_filters(1, stage1, w1, 1)
    mine = rows_of(r)

    def finish_two(h, value):
        x_hg[h, mine, :] = value.astype(jnp.bfloat16)

    norm(hid_b, moments_two, params[:, 2:3], params[:, 3:4], finish_two)
    gather_send(hg_at, g_send, g_recv)
    wait_exchange(1, lat_t, lat_b)
    moments_one = stats(lat_b)
    relay_filters(1, stage1, w1, 2)
    gather_relay(hg_at, g_send, g_recv)
    for off in range(3, depth):
        relay_filters(1, stage1, w1, off)
    gather_wait(hg_at, g_send, g_recv)
    wait_filters(1, f1_ref, w1)

    conv(x_hg, w1)

    def finish_one(h, value):
        out_b[h] = (x_cot[h, mine, :].astype(jnp.float32) + value).astype(jnp.bfloat16)

    norm(lat_b, moments_one, params[:, 0:1], params[:, 1:2], finish_one)
    for off in range(1, rows):
        to = lax.rem(r + off, rows)
        copy = remote(out_b.at[to], out_t.at[place(r)], o_send.at[to], o_recv.at[r], rows=to)
        copy.start()
        pending.append(copy)
    out_t[place(r)] = out_b[r]
    for off in range(1, rows):
        frm = lax.rem(r + off, rows)
        remote(out_b.at[frm], out_t.at[place(frm)], o_send.at[frm], o_recv.at[frm], rows=frm).wait_recv()
    out_ref[...] = out_t[...].reshape(channels, lanes).T
    for copy in pending:
        copy.wait_send()
    wait_z_sends(0, f2_ref, stage2)
    wait_z_sends(1, f1_ref, stage1)
    wait_piece_sends(0, f2_ref, w2)
    wait_piece_sends(1, f1_ref, w1)


def kernel_body(
    depth, rows,
    latent, hidden, cotangent, filter_one, filter_two, gain_one, shift_one, gain_two, shift_two,
):
    images, _, breadth, channels = latent.shape
    lanes = images * breadth
    block = channels // rows
    halves = rows // depth
    wide = -(-TAPS * block // 128) * 128
    bf16, f32 = jnp.bfloat16, jnp.float32
    dma = pltpu.SemaphoreType.DMA
    out = pl.pallas_call(
        functools.partial(kernel, depth, rows, breadth),
        out_shape=jax.ShapeDtypeStruct((lanes, channels), bf16),
        in_specs=[pl.BlockSpec(memory_space=pltpu.VMEM)] * 9,
        out_specs=pl.BlockSpec(memory_space=pltpu.VMEM),
        scratch_shapes=[
            pltpu.VMEM((rows, channels, lanes), bf16),
            pltpu.VMEM((rows, channels, lanes), bf16),
            pltpu.VMEM((channels, lanes), bf16),
            pltpu.VMEM((channels, lanes), bf16),
            pltpu.VMEM((rows, block, lanes), bf16),
            pltpu.VMEM((rows, block, lanes), bf16),
            pltpu.VMEM((depth, halves, block, wide), bf16),
            pltpu.VMEM((depth, halves, block, wide), bf16),
            pltpu.VMEM((rows, block, wide), bf16),
            pltpu.VMEM((rows, block, wide), bf16),
            pltpu.VMEM((wide, channels), bf16),
            pltpu.VMEM((rows, wide, lanes), f32),
            pltpu.VMEM((rows, block, lanes), f32),
            pltpu.VMEM((rows, block, lanes), bf16),
            pltpu.VMEM((rows, block, lanes), bf16),
            pltpu.VMEM((halves, block, wide), bf16),
            pltpu.VMEM((halves, block, wide), bf16),
            pltpu.VMEM((channels, 8), f32),
            dma((2, 2, depth, halves)), dma((2, depth, halves)),
            dma((2, rows)), dma((2, rows)),
            dma((rows,)), dma((rows,)),
            dma((rows,)), dma((rows,)),
            dma((2, rows)), dma((2, rows)),
            dma((rows,)), dma((rows,)),
        ],
        compiler_params=pltpu.CompilerParams(collective_id=0, has_side_effects=True),
    )(
        latent.reshape(lanes, channels), hidden.reshape(lanes, channels),
        cotangent.reshape(lanes, channels), filter_one, filter_two,
        gain_one, shift_one, gain_two, shift_two,
    )
    return out.reshape(latent.shape)


def solution(mesh):
    depth, rows = mesh.shape["dp"], mesh.shape["rows"]
    in_specs = (
        P("dp", "rows", None, None),
        P("dp", "rows", None, None),
        P("dp", "rows", None, None),
        P(None, "dp", "rows"),
        P(None, "dp", "rows"),
        P(),
        P(),
        P(),
        P(),
    )

    def body(latent, *rest):
        images, rows_here, breadth, channels = latent.shape
        fits = (
            rows_here == 1
            and images * breadth == 128
            and depth > 2
            and rows == 2 * depth
            and rows % 2 == 0
            and channels % (rows * GSIZE) == 0
            and (channels // rows) % 16 == 0
            and channels % 128 == 0
        )
        if fits:
            return kernel_body(depth, rows, latent, *rest)
        return plain_body(latent, *rest)

    return jax.shard_map(
        body, mesh=mesh, in_specs=in_specs, out_specs=P("dp", "rows", None, None), check_vma=False
    )
```

```python
import functools

import jax
import jax.numpy as jnp
from jax import lax
from jax.experimental import pallas as pl
from jax.experimental.pallas import tpu as pltpu
from jax.sharding import PartitionSpec as P

GROUPS = 16
GSIZE = 40
TAPS = 9
MESH = pl.DeviceIdType.MESH


def extended(block, sides, width):
    for axis, dim in sides:
        count = lax.axis_size(axis)
        forward = [(i, i + 1) for i in range(count - 1)]
        backward = [(target, source) for source, target in forward]
        low = lax.ppermute(
            lax.slice_in_dim(block, block.shape[dim] - width, None, axis=dim), axis, forward
        )
        high = lax.ppermute(lax.slice_in_dim(block, 0, width, axis=dim), axis, backward)
        block = jnp.concatenate([low, block, high], axis=dim)
    return block


def group_sums(values):
    per_channel = jnp.sum(values, axis=(1, 2))
    return jnp.sum(per_channel.reshape(per_channel.shape[0], GROUPS, -1), axis=2)


def expand_groups(moment):
    return jnp.repeat(moment, GSIZE, axis=1)[:, None, None, :]


def finish_stats(sum_plain, sum_square, number):
    average = sum_plain / number
    variance = sum_square / number - average * average
    return (average, lax.rsqrt(variance + 1e-05))


def reduced_stats(field, number):
    values = field.astype(jnp.float32)
    sum_plain, sum_square = lax.psum((group_sums(values), group_sums(values * values)), "rows")
    return finish_stats(sum_plain, sum_square, number)


def norm_backward(field, stats, gain, shift, incoming, number):
    average, inverse = stats
    values = field.astype(jnp.float32)
    normed = (values - expand_groups(average)) * expand_groups(inverse)
    linear = normed * gain + shift
    logistic = jax.nn.sigmoid(linear)
    scaled = incoming * logistic * (1.0 + linear * (1.0 - logistic)) * gain
    sum_first, sum_second = lax.psum((group_sums(scaled), group_sums(scaled * normed)), "rows")
    first = sum_first / number
    second = sum_second / number
    return expand_groups(inverse) * (scaled - expand_groups(first) - normed * expand_groups(second))


def conv_backward(gradient, weights):
    images, rows_here, breadth, channels = gradient.shape
    padded = extended(gradient, (("rows", 1),), 1)
    padded = jnp.pad(padded, ((0, 0), (0, 0), (1, 1), (0, 0)))
    pixels = images * rows_here * breadth
    shifted = []
    for tap_index in range(9):
        down_step = tap_index // 3 - 1
        side_step = tap_index % 3 - 1
        window = padded[
            :, 1 - down_step : 1 - down_step + rows_here, 1 - side_step : 1 - side_step + breadth, :
        ]
        shifted.append(window.reshape(pixels, channels))
    stacked = jnp.stack(shifted, axis=1)
    gathered = lax.all_gather(weights, "dp", axis=1, tiled=True)
    section = lax.all_gather(gathered, "rows", axis=2, tiled=True)
    columns = section.shape[2]
    window = stacked.reshape(pixels, 9 * columns)
    flat = jnp.transpose(section, (0, 2, 1)).reshape(9 * columns, section.shape[1])
    result = jnp.dot(window, flat, preferred_element_type=jnp.float32)
    return result.reshape(images, rows_here, breadth, channels)


def plain_body(
    latent, hidden, cotangent, filter_one, filter_two, gain_one, shift_one, gain_two, shift_two
):
    number = latent.shape[1] * lax.axis_size("rows") * latent.shape[2] * GSIZE
    stats_two = reduced_stats(hidden, number)
    back_two = conv_backward(cotangent, filter_two)
    hidden_grad = norm_backward(hidden, stats_two, gain_two, shift_two, back_two, number).astype(
        jnp.bfloat16
    )
    stats_one = reduced_stats(latent, number)
    back_one = conv_backward(hidden_grad, filter_one)
    latent_part = norm_backward(latent, stats_one, gain_one, shift_one, back_one, number)
    return (cotangent.astype(jnp.float32) + latent_part).astype(jnp.bfloat16)


def kernel(
    depth, rows, breadth,
    lat_ref, hid_ref, cot_ref, raw1, raw2, gain1, shift1, gain2, shift2,
    out_ref,
    x_cot, x_hg, lat_t, hid_t, lat_b, hid_b, stage1, stage2, w1, w2, wt, y_ref, back, out_b, out_t,
    f1_ref, f2_ref, par_ref,
    z_send, z_recv, w_send, w_recv, c_send, c_recv, g_send, g_recv,
    a_send, a_recv, o_send, o_recv,
):
    d = lax.axis_index("dp")
    r = lax.axis_index("rows")
    channels, lanes = x_cot.shape[1:]
    block = channels // rows
    images = lanes // breadth
    halves = rows // depth
    wide = w1.shape[2]
    number = rows * breadth * GSIZE

    def place(index):
        return index + lax.rem(index, 2) * (rows - 2 * index)

    def rows_of(index):
        return pl.ds(pl.multiple_of(place(index) * block, block), block)

    def arrange(raw, ready):
        for k in range(halves):
            ready[k, :, TAPS * block :] = jnp.zeros((block, wide - TAPS * block), jnp.bfloat16)
        for tap in range(TAPS):
            turned = raw[tap].T
            for k in range(halves):
                ready[k, :, tap * block : (tap + 1) * block] = turned[:, k * block : (k + 1) * block]

    def remote(src, dst, send, recv, **device):
        return pltpu.make_async_remote_copy(
            src_ref=src, dst_ref=dst, send_sem=send, recv_sem=recv,
            device_id=device, device_id_type=MESH,
        )

    barrier = pltpu.get_barrier_semaphore()
    for off in range(1, depth):
        pl.semaphore_signal(barrier, inc=1, device_id={"dp": lax.rem(d + off, depth)}, device_id_type=MESH)
    for off in range(1, rows):
        pl.semaphore_signal(barrier, inc=1, device_id={"rows": lax.rem(r + off, rows)}, device_id_type=MESH)

    arrange(raw2, f2_ref)
    x_cot[r] = cot_ref[...].T
    hid_t[...] = hid_ref[...].T
    lat_t[...] = lat_ref[...].T
    pl.semaphore_wait(barrier, depth - 1 + rows - 1)

    pending = []

    def z_hop(which, src, stage, origin, k, way):
        to = d + 1 - 2 * way
        return remote(
            src, stage.at[origin, k], z_send.at[which, way, origin, k], z_recv.at[which, origin, k], dp=to
        )

    def start_z(which, src, stage):
        for k in range(halves):
            @pl.when(d < depth - 1)
            def _():
                z_hop(which, src.at[k], stage, d, k, 0).start()

            @pl.when(d > 0)
            def _():
                z_hop(which, src.at[k], stage, d, k, 1).start()

    def wait_z_sends(which, src, stage):
        for origin in range(depth):
            for k in range(halves):
                @pl.when((d < depth - 1) & (origin <= d))
                def _():
                    z_hop(which, src.at[k], stage, origin, k, 0).wait_send()

                @pl.when((d > 0) & (origin >= d))
                def _():
                    z_hop(which, src.at[k], stage, origin, k, 1).wait_send()

    def start_exchange(which, src, dst):
        for off in range(1, rows):
            to = lax.rem(r + off, rows)
            copy = remote(
                src.at[rows_of(to), :], dst.at[r],
                a_send.at[which, to], a_recv.at[which, r], rows=to,
            )
            copy.start()
            pending.append(copy)
        dst[r] = src[rows_of(r), :]

    def wait_exchange(which, src, dst):
        for off in range(1, rows):
            frm = lax.rem(r + off, rows)
            remote(src.at[pl.ds(0, block), :], dst.at[frm], a_send.at[which, frm], a_recv.at[which, frm], rows=frm).wait_recv()

    def send_piece(which, origin, k, piece, w):
        to = place(origin * halves + k)

        @pl.when(to != r)
        def _():
            remote(piece, w.at[r], w_send.at[which, to], w_recv.at[which, r], rows=to).start()

        @pl.when(to == r)
        def _():
            w[r] = piece[...]

    def send_own(which, src, w):
        for k in range(halves):
            send_piece(which, d, k, src.at[k], w)

    def wait_piece_sends(which, src, w):
        for off in range(1, rows):
            to = lax.rem(r + off, rows)
            remote(src.at[0], w.at[r], w_send.at[which, to], w_recv.at[which, r], rows=to).wait_send()

    def relay_filters(which, stage, w, off):
        for k in range(halves):
            for way in range(2):
                origin = d - off if way == 0 else d + off

                @pl.when((origin >= 0) & (origin < depth))
                def _():
                    hop = z_hop(which, stage.at[origin, k], stage, origin, k, way)
                    hop.wait_recv()

                    @pl.when((d < depth - 1) if way == 0 else (d > 0))
                    def _():
                        hop.start()

                    send_piece(which, origin, k, stage.at[origin, k], w)

    def wait_filters(which, src, w):
        for off in range(1, rows):
            frm = lax.rem(r + off, rows)
            remote(src.at[0], w.at[frm], w_send.at[which, frm], w_recv.at[which, frm], rows=frm).wait_recv()

    parity = lax.rem(r, 2)
    sibling = r + 1 - 2 * parity

    def gather_send(at, send, recv):
        for off in range(1, rows // 2):
            to = lax.rem(r + 2 * off, rows)
            copy = remote(at(r), at(r), send.at[to], recv.at[r], rows=to)
            copy.start()
            pending.append(copy)
        copy = remote(at(r), at(r), send.at[sibling], recv.at[r], rows=sibling)
        copy.start()
        pending.append(copy)

    def gather_relay(at, send, recv):
        for off in range(1, rows // 2):
            frm = lax.rem(r + 2 * off, rows)
            remote(at(frm), at(frm), send.at[frm], recv.at[frm], rows=frm).wait_recv()
            twin = lax.rem(sibling + 2 * off, rows)
            copy = remote(at(frm), at(frm), send.at[twin], recv.at[frm], rows=sibling)
            copy.start()
            pending.append(copy)

    def gather_wait(at, send, recv):
        for off in range(0, rows // 2):
            frm = lax.rem(sibling + 2 * off, rows)
            remote(at(frm), at(frm), send.at[frm], recv.at[frm], rows=sibling).wait_recv()

    def cot_at(h):
        return x_cot.at[h]

    def hg_at(owner):
        return x_hg.at[:, rows_of(owner), :]

    start_z(0, f2_ref, stage2)
    gather_send(cot_at, c_send, c_recv)
    start_exchange(0, hid_t, hid_b)
    send_own(0, f2_ref, w2)
    arrange(raw1, f1_ref)
    raw_params = [p[...].reshape(1, channels) for p in (gain1, shift1, gain2, shift2)]
    par_ref[...] = jnp.concatenate(raw_params + raw_params, axis=0).T

    lane = lax.broadcasted_iota(jnp.int32, (1, lanes), 1)
    column = lax.rem(lane, breadth)
    image_of = lax.div(lane, breadth)
    groups = block // GSIZE

    def group_means(sums):
        per_lane = jnp.sum(sums.reshape(groups, GSIZE, lanes), axis=1)
        total = jnp.zeros_like(per_lane)
        for image in range(images):
            mine = image_of == image
            part = jnp.sum(jnp.where(mine, per_lane, 0.0), axis=1, keepdims=True)
            total = jnp.where(mine, part, total)
        total = total * (1.0 / number)
        return jnp.broadcast_to(total[:, None, :], (groups, GSIZE, lanes)).reshape(block, lanes)

    def stats(field):
        plain = jnp.zeros((block, lanes), jnp.float32)
        square = jnp.zeros((block, lanes), jnp.float32)
        for h in range(rows):
            values = field[h].astype(jnp.float32)
            plain += values
            square += values * values
        average = group_means(plain)
        variance = group_means(square) - average * average
        return average, lax.rsqrt(variance + 1e-05)

    params = par_ref[rows_of(r), :]

    def conv(x, w):
        wt[...] = w[...].reshape(channels, wide).T
        for h in range(0, rows, 2):
            pair = jnp.concatenate([x[h], x[h + 1]], axis=1)
            result = jnp.dot(wt[...], pair, preferred_element_type=jnp.float32)
            y_ref[h] = result[:, :lanes]
            y_ref[h + 1] = result[:, lanes:]

    def back_at(h):
        sums = []
        for side in range(3):
            total = None
            for down in range(3):
                source = h - (down - 1)
                if 0 <= source < rows:
                    tap = 3 * down + side
                    term = y_ref[source, tap * block : (tap + 1) * block, :]
                    total = term if total is None else total + term
            sums.append(total)
        left = jnp.where(column == breadth - 1, 0.0, pltpu.roll(sums[0], lanes - 1, 1))
        right = jnp.where(column == 0, 0.0, pltpu.roll(sums[2], 1, 1))
        return sums[1] + left + right

    def norm(field, moments, gain, shift, finish):
        average, inverse = moments
        sum_first = jnp.zeros((block, lanes), jnp.float32)
        sum_second = jnp.zeros((block, lanes), jnp.float32)
        for h in range(rows):
            normed = (field[h].astype(jnp.float32) - average) * inverse
            linear = normed * gain + shift
            logistic = 1.0 / (1.0 + jnp.exp(-linear))
            scaled = back_at(h) * logistic * (1.0 + linear * (1.0 - logistic)) * gain
            back[h] = scaled
            sum_first += scaled
            sum_second += scaled * normed
        first = group_means(sum_first)
        second = group_means(sum_second)
        for h in range(rows):
            normed = (field[h].astype(jnp.float32) - average) * inverse
            finish(h, inverse * (back[h] - first - normed * second))

    relay_filters(0, stage2, w2, 1)
    gather_relay(cot_at, c_send, c_recv)
    start_exchange(1, lat_t, lat_b)
    relay_filters(0, stage2, w2, 2)
    wait_exchange(0, hid_t, hid_b)
    moments_two = stats(hid_b)
    start_z(1, f1_ref, stage1)
    for off in range(3, depth):
        relay_filters(0, stage2, w2, off)
    gather_wait(cot_at, c_send, c_recv)
    wait_filters(0, f2_ref, w2)

    conv(x_cot, w2)
    send_own(1, f1_ref, w1)
    relay_filters(1, stage1, w1, 1)
    mine = rows_of(r)

    def finish_two(h, value):
        x_hg[h, mine, :] = value.astype(jnp.bfloat16)

    norm(hid_b, moments_two, params[:, 2:3], params[:, 3:4], finish_two)
    gather_send(hg_at, g_send, g_recv)
    wait_exchange(1, lat_t, lat_b)
    moments_one = stats(lat_b)
    relay_filters(1, stage1, w1, 2)
    for off in range(3, depth):
        relay_filters(1, stage1, w1, off)
    gather_relay(hg_at, g_send, g_recv)
    gather_wait(hg_at, g_send, g_recv)
    wait_filters(1, f1_ref, w1)

    conv(x_hg, w1)

    def finish_one(h, value):
        out_b[h] = (x_cot[h, mine, :].astype(jnp.float32) + value).astype(jnp.bfloat16)

    norm(lat_b, moments_one, params[:, 0:1], params[:, 1:2], finish_one)
    for off in range(1, rows):
        to = lax.rem(r + off, rows)
        copy = remote(out_b.at[to], out_t.at[place(r)], o_send.at[to], o_recv.at[r], rows=to)
        copy.start()
        pending.append(copy)
    out_t[place(r)] = out_b[r]
    for off in range(1, rows):
        frm = lax.rem(r + off, rows)
        remote(out_b.at[frm], out_t.at[place(frm)], o_send.at[frm], o_recv.at[frm], rows=frm).wait_recv()
    out_ref[...] = out_t[...].reshape(channels, lanes).T
    for copy in pending:
        copy.wait_send()
    wait_z_sends(0, f2_ref, stage2)
    wait_z_sends(1, f1_ref, stage1)
    wait_piece_sends(0, f2_ref, w2)
    wait_piece_sends(1, f1_ref, w1)


def kernel_body(
    depth, rows,
    latent, hidden, cotangent, filter_one, filter_two, gain_one, shift_one, gain_two, shift_two,
):
    images, _, breadth, channels = latent.shape
    lanes = images * breadth
    block = channels // rows
    halves = rows // depth
    wide = -(-TAPS * block // 128) * 128
    bf16, f32 = jnp.bfloat16, jnp.float32
    dma = pltpu.SemaphoreType.DMA
    out = pl.pallas_call(
        functools.partial(kernel, depth, rows, breadth),
        out_shape=jax.ShapeDtypeStruct((lanes, channels), bf16),
        in_specs=[pl.BlockSpec(memory_space=pltpu.VMEM)] * 9,
        out_specs=pl.BlockSpec(memory_space=pltpu.VMEM),
        scratch_shapes=[
            pltpu.VMEM((rows, channels, lanes), bf16),
            pltpu.VMEM((rows, channels, lanes), bf16),
            pltpu.VMEM((channels, lanes), bf16),
            pltpu.VMEM((channels, lanes), bf16),
            pltpu.VMEM((rows, block, lanes), bf16),
            pltpu.VMEM((rows, block, lanes), bf16),
            pltpu.VMEM((depth, halves, block, wide), bf16),
            pltpu.VMEM((depth, halves, block, wide), bf16),
            pltpu.VMEM((rows, block, wide), bf16),
            pltpu.VMEM((rows, block, wide), bf16),
            pltpu.VMEM((wide, channels), bf16),
            pltpu.VMEM((rows, wide, lanes), f32),
            pltpu.VMEM((rows, block, lanes), f32),
            pltpu.VMEM((rows, block, lanes), bf16),
            pltpu.VMEM((rows, block, lanes), bf16),
            pltpu.VMEM((halves, block, wide), bf16),
            pltpu.VMEM((halves, block, wide), bf16),
            pltpu.VMEM((channels, 8), f32),
            dma((2, 2, depth, halves)), dma((2, depth, halves)),
            dma((2, rows)), dma((2, rows)),
            dma((rows,)), dma((rows,)),
            dma((rows,)), dma((rows,)),
            dma((2, rows)), dma((2, rows)),
            dma((rows,)), dma((rows,)),
        ],
        compiler_params=pltpu.CompilerParams(collective_id=0, has_side_effects=True),
    )(
        latent.reshape(lanes, channels), hidden.reshape(lanes, channels),
        cotangent.reshape(lanes, channels), filter_one, filter_two,
        gain_one, shift_one, gain_two, shift_two,
    )
    return out.reshape(latent.shape)


def solution(mesh):
    depth, rows = mesh.shape["dp"], mesh.shape["rows"]
    in_specs = (
        P("dp", "rows", None, None),
        P("dp", "rows", None, None),
        P("dp", "rows", None, None),
        P(None, "dp", "rows"),
        P(None, "dp", "rows"),
        P(),
        P(),
        P(),
        P(),
    )

    def body(latent, *rest):
        images, rows_here, breadth, channels = latent.shape
        fits = (
            rows_here == 1
            and images * breadth == 128
            and depth > 2
            and rows == 2 * depth
            and rows % 2 == 0
            and channels % (rows * GSIZE) == 0
            and (channels // rows) % 16 == 0
            and channels % 128 == 0
        )
        if fits:
            return kernel_body(depth, rows, latent, *rest)
        return plain_body(latent, *rest)

    return jax.shard_map(
        body, mesh=mesh, in_specs=in_specs, out_specs=P("dp", "rows", None, None), check_vma=False
    )
```
